32 devices in a mesh: vocab: 16 (over z, y, x), seq: 2 (over core).
Axes of the slice: x: 2, y: 2, z: 4, core: 2. Of those that a mesh axis runs over, the one named last changes fastest.
Arguments:
- hidden_expert: bfloat16 [128, 8192], P('vocab', 'seq'), may hold values from -51 to 51
- hidden_amateur: bfloat16 [128, 4096], P('vocab', 'seq'), may hold values from -51 to 51
- gain_expert: bfloat16 [8192], P('seq'), may hold values from 0.5 to 1.5
- gain_amateur: bfloat16 [4096], P('seq'), may hold values from 0.5 to 1.5
- unembed_expert: bfloat16 [8192, 16384], P('seq', 'vocab'), may hold values from -0.31221253 to 0.31221253
- unembed_amateur: bfloat16 [4096, 16384], P('seq', 'vocab'), may hold values from -0.52734375 to 0.52734375
Outputs:
- scores: float32 [128, 16384], P('seq', 'vocab')
- lse_expert: float32 [128], P('seq')
- lse_amateur: float32 [128], P('seq')
The draws below stay inside these ranges and needn't reach their ends.
All inputs are finite; a program needn't handle non-finite values.
Results may differ from the reference program's by a relative error of at most 0.0017.
Values may be sent and summed in bfloat16 or wider, within the bound.
No kernel may reach another device: no remote copies, remote signals or barrier semaphores. Data moves between devices by JAX's collectives and lax.ppermute only.
A program may use at most 64 MiB of HBM per device.

```python
import jax
import jax.numpy as jnp
from jax import lax

DE = 8192
DA = 4096
VOCAB = 16384
SEQS = 128


def column_scale(width):
    return jnp.exp(jnp.log(3.0) * jnp.arange(width, dtype=jnp.float32) / width)


def draw_hidden_expert(key, part):
    model_key = jax.random.fold_in(key, 1)
    values = jax.random.truncated_normal(jax.random.fold_in(model_key, 7), -4.0, 4.0, (SEQS, DE), jnp.float32) * column_scale(DE)[None, :]
    return values.astype(jnp.bfloat16)


def draw_hidden_amateur(key, part):
    model_key = jax.random.fold_in(key, 2)
    values = jax.random.truncated_normal(jax.random.fold_in(model_key, 7), -4.0, 4.0, (SEQS, DA), jnp.float32) * column_scale(DA)[None, :]
    return values.astype(jnp.bfloat16)


def draw_unembed_expert(key, part):
    model_key = jax.random.fold_in(key, 1)
    base = jax.random.truncated_normal(jax.random.fold_in(model_key, 8), -5.0, 5.0, (DE, VOCAB), jnp.float32) * (3.0 / jnp.sqrt(float(DE)))
    return base.astype(jnp.bfloat16)


def draw_unembed_amateur(key, part):
    model_key = jax.random.fold_in(key, 2)
    base = jax.random.truncated_normal(jax.random.fold_in(model_key, 8), -5.0, 5.0, (DA, VOCAB), jnp.float32) * (3.0 / jnp.sqrt(float(DA)))
    return base.astype(jnp.bfloat16)


def setup_inputs(seed: int = 0) -> dict:
    key_of = jax.random.split(jax.random.key(seed), 7)
    return {
        "hidden_expert": draw_hidden_expert(jax.random.fold_in(key_of[6], 71), 0),
        "hidden_amateur": draw_hidden_amateur(jax.random.fold_in(key_of[6], 71), 0),
        "gain_expert": jnp.clip(1.0 + 0.1 * jax.random.normal(key_of[2], (DE,), jnp.float32), 0.5, 1.5).astype(jnp.bfloat16),
        "gain_amateur": jnp.clip(1.0 + 0.1 * jax.random.normal(key_of[3], (DA,), jnp.float32), 0.5, 1.5).astype(jnp.bfloat16),
        "unembed_expert": draw_unembed_expert(jax.random.fold_in(key_of[6], 71), 0),
        "unembed_amateur": draw_unembed_amateur(jax.random.fold_in(key_of[6], 71), 0),
    }


def project_model(hidden, gain, weight, width):
    values = hidden.astype(jnp.float32)
    scaled = (values * gain.astype(jnp.float32)).astype(jnp.bfloat16)
    inverse = lax.rsqrt(lax.optimization_barrier(jnp.sum(values * values, axis=1)) / width + 1e-05)
    return inverse[:, None] * jnp.dot(scaled, weight, preferred_element_type=jnp.float32)

def normalizer(logits):
    top = lax.optimization_barrier(jnp.max(logits, axis=1))
    return (top, top + jnp.log(lax.optimization_barrier(jnp.sum(jnp.exp(logits - top[:, None]), axis=1))))

def reference(hidden_expert, hidden_amateur, gain_expert, gain_amateur, unembed_expert, unembed_amateur):
    logits_expert = project_model(hidden_expert, gain_expert, unembed_expert, DE)
    logits_amateur = project_model(hidden_amateur, gain_amateur, unembed_amateur, DA)
    top_expert, lse_expert = normalizer(logits_expert)
    top_amateur, lse_amateur = normalizer(logits_amateur)
    logp_expert = logits_expert - lse_expert[:, None]
    logp_amateur = logits_amateur - lse_amateur[:, None]
    bound = top_expert - lse_expert + jnp.log(0.1)
    scores = logp_expert - logp_amateur + jnp.minimum(0.0, logp_expert - bound[:, None])
    return (scores, lse_expert, lse_amateur)
```

```python
import jax
import jax.numpy as jnp
from jax import lax
from jax.experimental import pallas as pl
from jax.experimental.pallas import tpu as pltpu
from jax.sharding import PartitionSpec as P


LANES = 128


def span(stages, parity):
    out = [0]
    for stage in stages:
        out = out + [mask[parity] ^ have for mask in stage for have in out]
    return out


def widen_stages(shards):
    bits = shards.bit_length() - 1
    near, far = min(bits, 2), min(max(bits - 2, 0), 2)
    stages = []
    if far:
        stages.append([(m << 2, m << 2) for m in ([2, 3, 1] if far == 2 else [1])])
    stages += [[(1 << b, 1 << b)] for b in range(4, bits)]
    stages += [[(1, 2)], [(2, 1)]] if near == 2 else [[(1 << b, 1 << b)] for b in range(near)]
    return stages


def stat_stages(shards):
    bits = shards.bit_length() - 1
    stages = []
    for low in range(0, bits, 2):
        width = min(2, bits - low)
        stages.append([(m << low, m << low) for m in range(1, 1 << width)])
    return stages


def shift(x, mask, shards, parts):
    pairs = [(v * parts + c, (v ^ mask[c % 2]) * parts + c) for v in range(shards) for c in range(parts)]
    return lax.ppermute(x, ("vocab", "seq"), pairs)


def widen(x, stages, shards, parts):
    pieces = [x]
    for stage in stages:
        have = pieces[0] if len(pieces) == 1 else jnp.concatenate(pieces, axis=0)
        pieces = [have] + [shift(have, mask, shards, parts) for mask in stage]
    return pieces


def project(pieces, gain, weight, stages, shards, parts):
    width, vocab = weight.shape
    rows = sum(p.shape[0] for p in pieces)
    group = rows // shards
    distances = [span(stages, parity) for parity in range(2)]
    block = min(512, width)
    steps = width // block
    count = len(pieces)
    halves = parts == 2
    full = (rows, vocab + LANES)
    outs = [(rows // 2, vocab + LANES)] * 2 if halves else [full]

    def kernel(*refs):
        piece_refs, (gain_ref, weight_ref) = refs[:count], refs[count : count + 2]
        out_refs = refs[count + 2 : count + 2 + len(outs)]
        lhs, acc, buffer, sems = refs[count + 2 + len(outs) :]

        def copy(k):
            return pltpu.make_async_copy(weight_ref.at[pl.ds(k * block, block)], buffer.at[k], sems.at[k])

        for k in range(steps):
            copy(k).start()
        start = 0
        for ref in piece_refs:
            size = ref.shape[0]
            values = ref[...].astype(jnp.float32)
            lhs[start : start + size, :] = (values * gain_ref[...].astype(jnp.float32)).astype(jnp.bfloat16)
            squares = values * values
            total = squares[:, :LANES]
            for lane in range(LANES, width, LANES):
                total = total + squares[:, lane : lane + LANES]
            acc[start : start + size, vocab:] = total
            start += size
        for k in range(steps):
            copy(k).wait()
            part = jnp.dot(lhs[:, k * block : (k + 1) * block], buffer[k], preferred_element_type=jnp.float32)
            if k == 0:
                acc[:, :vocab] = part
            else:
                acc[:, :vocab] += part
        shard = lax.axis_index("vocab")
        core = lax.axis_index("seq")
        odd = core % 2
        for j in range(shards):
            there = shard ^ jnp.where(odd == 1, distances[1][j], distances[0][j])
            value = acc[j * group : (j + 1) * group, :]
            if halves:
                there = there ^ (core * (shards // 2))
                inside = there < shards // 2
                row = pl.multiple_of((there % (shards // 2)) * group, group)

                @pl.when(inside)
                def _():
                    out_refs[0][pl.ds(row, group), :] = value

                @pl.when(jnp.logical_not(inside))
                def _():
                    out_refs[1][pl.ds(row, group), :] = value
            else:
                row = pl.multiple_of(there * group, group)
                out_refs[0][pl.ds(row, group), :] = value

    vmem = pl.BlockSpec(memory_space=pltpu.VMEM)
    return pl.pallas_call(
        kernel,
        out_shape=[jax.ShapeDtypeStruct(o, jnp.float32) for o in outs],
        in_specs=[vmem] * (count + 1) + [pl.BlockSpec(memory_space=pl.ANY)],
        out_specs=[vmem] * len(outs),
        scratch_shapes=[
            pltpu.VMEM((rows, width), jnp.bfloat16),
            pltpu.VMEM(full, jnp.float32),
            pltpu.VMEM((steps, block, vocab), jnp.bfloat16),
            pltpu.SemaphoreType.DMA((steps,)),
        ],
        compiler_params=pltpu.CompilerParams(vmem_limit_bytes=40 << 20),
        cost_estimate=pl.CostEstimate(
            flops=2 * rows * width * vocab, bytes_accessed=2 * width * vocab, transcendentals=0
        ),
        name="project",
    )(*pieces, gain.reshape(1, width), weight)


def fold(outs, parts):
    if parts == 2:
        keep, send = outs
        return [keep, lax.ppermute(send, "seq", [(0, 1), (1, 0)])]
    return [lax.psum_scatter(outs[0], "seq", scatter_dimension=0, tiled=True)]


def columns(values):
    rows = values[0].shape[0]
    lane = lax.broadcasted_iota(jnp.int32, (rows, LANES), 1)
    block = jnp.zeros((rows, LANES), jnp.float32)
    for i, value in enumerate(values):
        block = jnp.where(lane == i, value, block)
    return jnp.transpose(block)[:8, :]


def local_stats(terms_expert, terms_amateur, width_expert, width_amateur):
    rows, vocab = terms_expert[0].shape[0], terms_expert[0].shape[1] - LANES
    count = len(terms_expert)

    def kernel(*refs):
        outs = refs[2 * count :]
        values = []
        for model, width in enumerate((width_expert, width_amateur)):
            terms = refs[model * count : (model + 1) * count]
            total = terms[0][...]
            for term in terms[1:]:
                total = total + term[...]
            squares = jnp.sum(total[:, vocab:], axis=1, keepdims=True)
            logits = lax.rsqrt(squares / width + 1e-05) * total[:, :vocab]
            outs[model][...] = logits
            top = jnp.max(logits, axis=1, keepdims=True)
            values += [top, jnp.sum(jnp.exp(logits - top), axis=1, keepdims=True)]
        outs[2][...] = columns(values)

    vmem = pl.BlockSpec(memory_space=pltpu.VMEM)
    return pl.pallas_call(
        kernel,
        out_shape=[
            jax.ShapeDtypeStruct((rows, vocab), jnp.float32),
            jax.ShapeDtypeStruct((rows, vocab), jnp.float32),
            jax.ShapeDtypeStruct((8, rows), jnp.float32),
        ],
        in_specs=[vmem] * (2 * count),
        out_specs=[vmem] * 3,
        compiler_params=pltpu.CompilerParams(vmem_limit_bytes=24 << 20),
        name="local_stats",
    )(*terms_expert, *terms_amateur)


def finish(logits_expert, logits_amateur, pieces, stages, shards):
    rows, vocab = logits_expert.shape
    count = len(pieces)
    distances = [span(stages, parity) for parity in range(2)]

    def kernel(*refs):
        expert_ref, amateur_ref = refs[:2]
        piece_refs = refs[2 : 2 + count]
        scores_ref, lse_expert_ref, lse_amateur_ref = refs[2 + count : 5 + count]
        table = refs[5 + count]
        shard = lax.axis_index("vocab")
        odd = lax.axis_index("seq") % 2
        j = 0
        for ref in piece_refs:
            for i in range(ref.shape[0] // 8):
                there = shard ^ jnp.where(odd == 1, distances[1][j], distances[0][j])
                table[pl.ds(pl.multiple_of(there * 8, 8), 8), :] = ref[i * 8 : (i + 1) * 8, :]
                j += 1
        block = table[0:8, :]
        tops = block
        for s in range(1, shards):
            tops = jnp.maximum(tops, table[s * 8 : s * 8 + 8, :])
        lses = []
        for model in range(2):
            top = tops[2 * model : 2 * model + 1, :]
            total = jnp.zeros_like(top)
            for s in range(shards):
                base = s * 8 + 2 * model
                total = total + table[base + 1 : base + 2, :] * jnp.exp(table[base : base + 1, :] - top)
            lses.append(top + jnp.log(total))
        lse_expert_ref[...] = lses[0]
        lse_amateur_ref[...] = lses[1]
        bound = tops[0:1, :] - lses[0] + jnp.log(0.1)
        wide = jnp.concatenate([lses[0], lses[1], bound, jnp.zeros((5, rows), jnp.float32)], axis=0)
        turned = jnp.transpose(wide)
        logp_expert = expert_ref[...] - turned[:, 0:1]
        logp_amateur = amateur_ref[...] - turned[:, 1:2]
        scores_ref[...] = logp_expert - logp_amateur + jnp.minimum(0.0, logp_expert - turned[:, 2:3])

    vmem = pl.BlockSpec(memory_space=pltpu.VMEM)
    scores, lse_expert, lse_amateur = pl.pallas_call(
        kernel,
        out_shape=[
            jax.ShapeDtypeStruct((rows, vocab), jnp.float32),
            jax.ShapeDtypeStruct((1, rows), jnp.float32),
            jax.ShapeDtypeStruct((1, rows), jnp.float32),
        ],
        in_specs=[vmem] * (2 + count),
        out_specs=[vmem] * 3,
        scratch_shapes=[pltpu.VMEM((shards * 8, rows), jnp.float32)],
        compiler_params=pltpu.CompilerParams(vmem_limit_bytes=24 << 20),
        name="finish",
    )(logits_expert, logits_amateur, *pieces)
    return scores, lse_expert.reshape(rows), lse_amateur.reshape(rows)


def solution(mesh):
    shards, parts = mesh.shape["vocab"], mesh.shape["seq"]
    stages, stats = widen_stages(shards), stat_stages(shards)

    def body(hidden_expert, hidden_amateur, gain_expert, gain_amateur, unembed_expert, unembed_amateur):
        width_expert, width_amateur = (x.shape[1] * parts for x in (hidden_expert, hidden_amateur))
        pieces_expert = widen(hidden_expert, stages, shards, parts)
        pieces_amateur = widen(hidden_amateur, stages, shards, parts)
        terms_amateur = fold(project(pieces_amateur, gain_amateur, unembed_amateur, stages, shards, parts), parts)
        terms_expert = fold(project(pieces_expert, gain_expert, unembed_expert, stages, shards, parts), parts)
        logits_expert, logits_amateur, block = local_stats(terms_expert, terms_amateur, width_expert, width_amateur)
        pieces = widen(block, stats, shards, parts)
        return finish(logits_expert, logits_amateur, pieces, stats, shards)

    return jax.shard_map(
        body,
        mesh=mesh,
        in_specs=(
            P("vocab", "seq"),
            P("vocab", "seq"),
            P("seq"),
            P("seq"),
            P("seq", "vocab"),
            P("seq", "vocab"),
        ),
        out_specs=(P("seq", "vocab"), P("seq"), P("seq")),
        check_vma=False,
    )
```
